256 devices in a mesh: pair: 128 (over x_hi, z, y, core), ao: 2 (over x_lo).
Axes of the slice: x: 4 (x_hi: 2, x_lo: 2; x = x_hi * 2 + x_lo), y: 4, z: 8, core: 2. Of those that a mesh axis runs over, the one named last changes fastest.
Arguments:
- gamma: bfloat16 [128, 1792, 1792], P('pair', 'ao'), may hold values from -6 to 6
- c_vir: bfloat16 [1024, 1792], replicated, may hold values from -0.125 to 0.125
- c_occ: bfloat16 [1024, 256], replicated, may hold values from -1.796875 to 1.796875
- pair_list: int32 [128, 2], replicated, may hold values from 0 to 255
- shell_order: int32 [128], replicated, may hold values from 0 to 127, each once
Outputs:
- ao_density: bfloat16 [1024, 1024], P('ao', 'pair')
The draws below stay inside these ranges and needn't reach their ends.
Inputs may be any that keep to these rules, and one draw needn't show every extreme that they name: shell_order holds each of 0 to 127 once.
All inputs are finite; a program needn't handle non-finite values.
Results may differ from the reference program's by a relative error of at most 0.0049.
Values sent between devices are 32-bit elements; how exact they have to be, the bound alone decides.
No kernel may reach another device: no remote copies, remote signals or barrier semaphores. Data moves between devices by JAX's collectives and lax.ppermute only.
A program may use at most 64 MiB of HBM per device.

```python
import jax
import jax.numpy as jnp
from jax import lax

NBF = 1024
V = 1792
OCC = 256
SB = 8
PAIRS = 128
SHELLS = 128


def touch_ends(drawn, key, least, high):
    shape = drawn.shape
    spot = [jax.random.randint(jax.random.fold_in(key, axis), (), 0, shape[axis]) for axis in range(len(shape))]
    drawn = drawn.at[tuple(spot)].set(least)
    longest = shape.index(max(shape))
    spot[longest] = (spot[longest] + 1) % shape[longest]
    return drawn.at[tuple(spot)].set(high)


def level_of(key, extent, shards, smallest, high):
    factor_of, own = 1.0, jax.random.fold_in(key, 6)
    for position, shards_of in shards:
        heights = jnp.exp(jax.random.uniform(jax.random.fold_in(own, position), (shards_of,), jnp.float32, smallest / len(shards), high / len(shards)))
        factor_of = factor_of * jnp.repeat(heights, extent[position] // shards_of).reshape([-1 if axis == position else 1 for axis in range(len(extent))])
    return factor_of


def normal_values(rng, dims, scale, limit, cuts=(), kind=jnp.bfloat16):
    drawn = scale * jax.random.normal(rng, dims, jnp.float32)
    if cuts:
        drawn = drawn * level_of(rng, dims, cuts, -0.22, 0.18)
    return jnp.clip(drawn, -limit, limit).astype(kind)


def setup_inputs(seed: int = 0) -> dict:
    splits = jax.random.split(jax.random.key(seed), 6)
    return {
        "gamma": normal_values(splits[0], (PAIRS, V, V), 1.0, 6.0, ((0, 128), (1, 2))),
        "c_vir": normal_values(splits[1], (NBF, V), V ** -0.5, 0.125),
        "c_occ": normal_values(splits[2], (NBF, OCC), 0.3, 1.796875),
        "pair_list": touch_ends(jax.random.randint(splits[3], (PAIRS, 2), 0, OCC), jax.random.fold_in(splits[3], 1), 0, OCC - 1).astype(jnp.int32),
        "shell_order": jax.random.permutation(splits[4], SHELLS).astype(jnp.int32),
    }


def reference(gamma, c_vir, c_occ, pair_list, shell_order):
    offsets = jnp.arange(SB, dtype=jnp.int32)
    row_index = (shell_order[:, None].astype(jnp.int32) * SB + offsets[None, :]).reshape(-1)
    vir_sorted = c_vir[row_index]
    occ_sorted = c_occ[row_index]

    def add_pair(total, inputs):
        amplitude, pair_ids = inputs
        half_block = lax.dot_general(amplitude, c_vir, (((1,), (1,)), ((), ())),
                                     preferred_element_type=jnp.float32).astype(jnp.bfloat16)
        ao_block = lax.dot_general(half_block, vir_sorted, (((0,), (1,)), ((), ())),
                                   preferred_element_type=jnp.float32)
        left_weight = occ_sorted[:, pair_ids[0]].astype(jnp.float32)
        right_weight = c_occ[:, pair_ids[1]].astype(jnp.float32)
        return total + right_weight[:, None] * ao_block * left_weight[None, :], None

    total, _ = lax.scan(add_pair, jnp.zeros((NBF, NBF), jnp.float32), (gamma, pair_list))
    return total.astype(jnp.bfloat16)
```

```python
import functools

import jax
import jax.numpy as jnp
from jax import lax
from jax.experimental import pallas as pl
from jax.experimental.pallas import tpu as pltpu
from jax.sharding import Mesh, PartitionSpec as P

SB = 8
TILE = 256
AXES = ("xh", "z", "y", "core", "xl")
NT = (((1,), (1,)), ((), ()))


def amplitude_kernel(where_ref, order_ref, pairs_ref, gamma_hbm, vir_hbm, occ_ref,
                     keep_hbm, send_hbm, gamma, vir, half, left, right, units, slot,
                     gamma_sem, vir_sem, out_sem):
    shells = order_ref.shape[0]
    rows_a = gamma.shape[0]
    step_a = rows_a // 4
    nu_tiles = vir.shape[0] // TILE

    def load_gamma(i):
        part = pl.ds(i * step_a, step_a)
        return pltpu.make_async_copy(gamma_hbm.at[part], gamma.at[part], gamma_sem.at[i])

    def load_vir(j):
        part = pl.ds(j * TILE, TILE)
        return pltpu.make_async_copy(vir_hbm.at[part], vir.at[part], vir_sem.at[j])

    load_vir(0).start()
    for i in range(4):
        load_gamma(i).start()
    for j in range(1, nu_tiles):
        load_vir(j).start()

    my_pair, my_ao, my_core = where_ref[0], where_ref[1], where_ref[2]

    def place(k, _):
        core = k % 2
        y = (k // 2) % 4
        z = (k // 8) % 8
        x = (k // 64) * 2
        x_first = (x * 4 + y) * 8 + z
        y_first = (y * 4 + x) * 8 + z
        base = jnp.where(core == my_core, 0, shells) + jnp.where(core == 0, x_first, y_first)
        shell = order_ref[k]
        slot[0, shell] = base
        slot[1, shell] = base + jnp.where(core == 0, 32, 8)
        return _

    lax.fori_loop(0, shells, place, 0, unroll=4)

    occ = occ_ref[...]
    occupied = occ.shape[1]
    pick_i = lax.broadcasted_iota(jnp.int32, (occupied, 128), 0) == pairs_ref[0, my_pair]
    left[...] = jnp.dot(occ, pick_i.astype(jnp.bfloat16), preferred_element_type=jnp.float32)
    pick_j = lax.broadcasted_iota(jnp.int32, (SB, occupied), 1) == pairs_ref[1, my_pair]
    right[...] = lax.dot_general(pick_j.astype(jnp.bfloat16), occ, NT, preferred_element_type=jnp.float32)

    local = pl.ds(pl.multiple_of(my_ao * rows_a, 128), rows_a)
    load_vir(0).wait()
    for j in range(nu_tiles):
        nu = pl.ds(j * TILE, TILE)
        if j == 0:
            for i in range(4):
                load_gamma(i).wait()
                part = pl.ds(i * step_a, step_a)
                half[part] = lax.dot_general(
                    gamma[part], vir[nu], NT, preferred_element_type=jnp.float32
                ).astype(jnp.bfloat16)
            for t in range(1, nu_tiles):
                load_vir(t).wait()
        else:
            half[...] = lax.dot_general(
                gamma[...], vir[nu], NT, preferred_element_type=jnp.float32
            ).astype(jnp.bfloat16)
        block = jnp.dot(vir[:, local], half[...], preferred_element_type=jnp.float32)
        weight = right[:, nu]
        columns = pl.ds((j % 2) * TILE, TILE)
        for s in range(shells):
            rows = slice(s * SB, (s + 1) * SB)
            scale = left[rows]
            units[slot[j // 2, s], :, columns] = (
                block[rows] * jnp.concatenate([scale, scale], axis=1) * weight
            )
    copies = [
        pltpu.make_async_copy(units.at[pl.ds(shells, shells)], send_hbm, out_sem.at[0]),
        pltpu.make_async_copy(units.at[pl.ds(0, shells)], keep_hbm, out_sem.at[1]),
    ]
    for copy in copies:
        copy.start()
    for copy in copies:
        copy.wait()


def weighted_blocks(where, order, pairs, gamma, vir, occ):
    basis, orbitals = vir.shape
    rows_a = gamma.shape[0]
    shells = order.shape[0]
    width = basis // 2
    out = jax.ShapeDtypeStruct((shells, SB, width), jnp.float32)
    smem = pl.BlockSpec(memory_space=pltpu.SMEM)
    hbm = pl.BlockSpec(memory_space=pl.ANY)
    return pl.pallas_call(
        amplitude_kernel,
        out_shape=(out, out),
        in_specs=[smem, smem, smem, hbm, hbm, pl.BlockSpec(memory_space=pltpu.VMEM)],
        out_specs=(hbm, hbm),
        scratch_shapes=[
            pltpu.VMEM((rows_a, orbitals), jnp.bfloat16),
            pltpu.VMEM((basis, orbitals), jnp.bfloat16),
            pltpu.VMEM((rows_a, TILE), jnp.bfloat16),
            pltpu.VMEM((basis, 128), jnp.float32),
            pltpu.VMEM((SB, basis), jnp.float32),
            pltpu.VMEM((2 * shells, SB, width), jnp.float32),
            pltpu.SMEM((2, shells), jnp.int32),
            pltpu.SemaphoreType.DMA((4,)),
            pltpu.SemaphoreType.DMA((basis // TILE,)),
            pltpu.SemaphoreType.DMA((2,)),
        ],
        compiler_params=pltpu.CompilerParams(vmem_limit_bytes=40 * 2**20),
        cost_estimate=pl.CostEstimate(
            flops=2 * rows_a * basis * (orbitals + basis),
            bytes_accessed=2 * (rows_a + basis) * orbitals + 4 * basis * basis,
            transcendentals=0,
        ),
        name="weighted_blocks",
    )(where, order, pairs, gamma, vir, occ)


def device(x, y, z, core):
    return ((((x // 2) * 8 + z) * 4 + y) * 2 + core) * 2 + x % 2


def shifted(step, ways):
    moves = []
    for x in range(4):
        for y in range(4):
            for z in range(8):
                for core in range(2):
                    to = {"x": x, "y": y, "z": z}
                    name = ways[core]
                    to[name] = (to[name] + step) % (8 if name == "z" else 4)
                    moves.append((device(x, y, z, core), device(core=core, **to)))
    return moves


def exchanged(value, ways, steps):
    count = value.shape[0]
    name = {"x": 2 * lax.axis_index("xh") + lax.axis_index("xl"), "y": lax.axis_index("y"), "z": lax.axis_index("z")}
    core = lax.axis_index("core")
    here = jnp.where(core == 0, name[ways[0]], name[ways[1]])
    total = lax.dynamic_index_in_dim(value, here, 0, keepdims=False)
    for step in steps:
        part = lax.dynamic_index_in_dim(value, (here + step) % count, 0, keepdims=False)
        total = total + lax.ppermute(part, AXES, shifted(step, ways))
    return total


def shards(gamma, c_vir, c_occ, pair_list, shell_order):
    own_pair = lax.axis_index(("xh", "z", "y", "core"))
    where = jnp.stack([own_pair, lax.axis_index("xl"), lax.axis_index("core")]).astype(jnp.int32)
    keep, send = weighted_blocks(where, shell_order, pair_list.T, gamma[0], c_vir, c_occ)
    total = keep + lax.ppermute(send, "core", [(0, 1), (1, 0)])
    total = total.reshape(4, 32, *total.shape[1:])
    total = exchanged(total, ("x", "y"), (1, 3, 2))
    total = total.reshape(4, 8, *total.shape[1:])
    total = exchanged(total, ("y", "x"), (1, 3, 2))
    total = jnp.sum(lax.all_to_all(total, "z", 0, 0, tiled=True), axis=0)
    return total.T.astype(jnp.bfloat16)


def solution(mesh):
    inner = Mesh(mesh.devices.reshape(2, 8, 4, 2, 2), AXES)
    pair = ("xh", "z", "y", "core")
    return jax.shard_map(
        shards,
        mesh=inner,
        in_specs=(P(pair, "xl", None), P(), P(), P(), P()),
        out_specs=P("xl", pair),
        check_vma=False,
    )
```

```python
import functools

import jax
import jax.numpy as jnp
from jax import lax
from jax.experimental import pallas as pl
from jax.experimental.pallas import tpu as pltpu
from jax.sharding import Mesh, PartitionSpec as P


SB = 8
AXES = ("xh", "z", "y", "core", "xl")
NT = (((1,), (1,)), ((), ()))
VMEM = pl.BlockSpec(memory_space=pltpu.VMEM)
SMEM = pl.BlockSpec(memory_space=pltpu.SMEM)
HBM = pl.BlockSpec(memory_space=pltpu.HBM)
QUARTER = 256
BATCH = 32


def mm(a, b, dims=(((1,), (0,)), ((), ()))):
    return lax.dot_general(a, b, dims, preferred_element_type=jnp.float32)


def slot_of(m, core):
    x_first = (m // 32) * 64 + m % 32
    y_first = (m // 8) * 16 + m % 8
    return jnp.where(core == 0, x_first, y_first)


def pair_of(m, core):
    x_first = (((m // 32) * 8 + m % 8) * 4 + (m // 8) % 4) * 2
    y_first = (((m // 8 % 2) * 8 + m % 8) * 4 + m // 16) * 2 + 1
    return jnp.where(core == 0, x_first, y_first)


def weighted(core, local, half, left, right, keep, send):
    shells = local.shape[0] // SB // 2
    for group, (out, owner) in enumerate(((send, 1 - core), (keep, core))):
        far = jnp.where(owner == 0, 32, 8)
        for m in range(shells):
            if m % BATCH == 0:
                block = mm(local[pl.ds((group * shells + m) * SB, BATCH * SB)], half[...])
            rows = slice(m % BATCH * SB, (m % BATCH + 1) * SB)
            scale = left[pl.ds((group * shells + m) * SB, SB)]
            scale = jnp.concatenate([scale, scale], axis=1)
            slot = slot_of(m, owner)
            out[slot] = block[rows, :QUARTER] * scale * right[:, :QUARTER]
            out[slot + far] = block[rows, QUARTER:] * scale * right[:, QUARTER:]


def first_kernel(where_ref, order_hbm, pairs_hbm, gamma_hbm, vir_hbm, occ_hbm,
                 keep, send, gamma, vir, local, left, right,
                 half, left_plain, occ_ref, order_ref, pairs_ref, gamma_sem, vir_sem, small_sem):
    rows_a = gamma.shape[0]
    cuts = ((0, rows_a // 4), (rows_a // 4, rows_a // 4), (rows_a // 2, rows_a // 2))

    def load_gamma(i):
        part = pl.ds(*cuts[i])
        return pltpu.make_async_copy(gamma_hbm.at[part], gamma.at[part], gamma_sem.at[i])

    def load_vir(j):
        source = (0, 2, 1, 3)[j]
        return pltpu.make_async_copy(
            vir_hbm.at[pl.ds(source * QUARTER, QUARTER)], vir.at[pl.ds(j * QUARTER, QUARTER)], vir_sem.at[j]
        )

    small = [
        pltpu.make_async_copy(source, to, small_sem.at[i])
        for i, (source, to) in enumerate(((pairs_hbm, pairs_ref), (occ_hbm, occ_ref), (order_hbm, order_ref)))
    ]
    for copy in small:
        copy.start()
    copies = [load_vir(0), load_gamma(0), load_vir(1), load_gamma(1), load_gamma(2), load_vir(2), load_vir(3)]
    for copy in copies:
        copy.start()

    my_pair, my_ao, core = where_ref[0], where_ref[1], where_ref[2]
    for copy in small:
        copy.wait()
    occ = occ_ref[...]
    occupied = occ.shape[1]
    pick_i = lax.broadcasted_iota(jnp.int32, (occupied, 128), 0) == pairs_ref[0, my_pair]
    left_plain[...] = mm(occ, pick_i.astype(jnp.bfloat16))
    pick_j = lax.broadcasted_iota(jnp.int32, (SB, occupied), 1) == pairs_ref[1, my_pair]
    pick_j = pick_j.astype(jnp.bfloat16)
    for j in range(4):
        source = (0, 2, 1, 3)[j]
        right[:, pl.ds(j * QUARTER, QUARTER)] = mm(pick_j, occ_ref[pl.ds(source * QUARTER, QUARTER)], NT)

    load_vir(0).wait()
    load_vir(1).wait()
    nu = pl.ds(0, 2 * QUARTER)
    for i, cut in enumerate(cuts):
        load_gamma(i).wait()
        half[pl.ds(*cut)] = mm(gamma[pl.ds(*cut)], vir[nu], NT).astype(jnp.bfloat16)
    load_vir(2).wait()
    load_vir(3).wait()

    columns = pl.ds(pl.multiple_of(my_ao * rows_a, 128), rows_a)
    shells = order_ref.shape[0] // 2
    for group, owner in enumerate((1 - core, core)):
        for m in range(shells):
            shell = order_ref[pair_of(m, owner)]
            quarter = shell // 32
            where = jnp.where(quarter == 1, 2, jnp.where(quarter == 2, 1, quarter)) * 32 + shell % 32
            to = pl.ds((group * shells + m) * SB, SB)
            local[to] = vir[pl.ds(pl.multiple_of(where * SB, SB), SB), columns]
            left[to] = left_plain[pl.ds(pl.multiple_of(shell * SB, SB), SB)]
    weighted(core, local, half, left, right[:, nu], keep, send)


def second_kernel(where_ref, gamma, vir, local, left, right, keep, send, half):
    nu = pl.ds(2 * QUARTER, 2 * QUARTER)
    half[...] = mm(gamma[...], vir[nu], NT).astype(jnp.bfloat16)
    weighted(where_ref[2], local, half, left, right[:, nu], keep, send)


def weighted_blocks(where, order, pairs, gamma, vir, occ):
    basis, orbitals = vir.shape
    rows_a = gamma.shape[0]
    shells = order.shape[0]
    out = jax.ShapeDtypeStruct((shells, SB, QUARTER), jnp.float32)
    half = pltpu.VMEM((rows_a, 2 * QUARTER), jnp.bfloat16)
    params = pltpu.CompilerParams(vmem_limit_bytes=24 * 2**20)
    work = pl.CostEstimate(
        flops=rows_a * basis * (orbitals + basis),
        bytes_accessed=2 * (rows_a + basis) * orbitals + 2 * basis * basis,
        transcendentals=0,
    )
    order, pairs, gamma, vir, occ = (
        pltpu.with_memory_space_constraint(x, pltpu.HBM) for x in (order, pairs, gamma, vir, occ)
    )
    keep0, send0, *held = pl.pallas_call(
        first_kernel,
        out_shape=(
            out,
            out,
            jax.ShapeDtypeStruct((rows_a, orbitals), jnp.bfloat16),
            jax.ShapeDtypeStruct((basis, orbitals), jnp.bfloat16),
            jax.ShapeDtypeStruct((basis, rows_a), jnp.bfloat16),
            jax.ShapeDtypeStruct((basis, 128), jnp.float32),
            jax.ShapeDtypeStruct((SB, basis), jnp.float32),
        ),
        in_specs=[SMEM] + [HBM] * 5,
        out_specs=(VMEM,) * 7,
        scratch_shapes=[
            half,
            pltpu.VMEM((basis, 128), jnp.float32),
            pltpu.VMEM(occ.shape, jnp.bfloat16),
            pltpu.SMEM(order.shape, jnp.int32),
            pltpu.SMEM(pairs.shape, jnp.int32),
            pltpu.SemaphoreType.DMA((3,)),
            pltpu.SemaphoreType.DMA((4,)),
            pltpu.SemaphoreType.DMA((3,)),
        ],
        compiler_params=params,
        cost_estimate=work,
        name="first_columns",
    )(where, order, pairs, gamma, vir, occ)
    keep1, send1 = pl.pallas_call(
        second_kernel,
        out_shape=(out, out),
        in_specs=[SMEM] + [VMEM] * 5,
        out_specs=(VMEM, VMEM),
        scratch_shapes=[half],
        compiler_params=params,
        cost_estimate=work,
        name="second_columns",
    )(where, *held)
    return keep0, send0, keep1, send1


def device(x, y, z, core):
    return ((((x // 2) * 8 + z) * 4 + y) * 2 + core) * 2 + x % 2


def shifted(step, ways):
    moves = []
    for x in range(4):
        for y in range(4):
            for z in range(8):
                for core in range(2):
                    to = {"x": x, "y": y, "z": z}
                    name = ways[core]
                    to[name] = (to[name] + step) % 4
                    moves.append((device(x, y, z, core), device(core=core, **to)))
    return moves


def exchanged(value, ways, steps):
    name = {"x": 2 * lax.axis_index("xh") + lax.axis_index("xl"), "y": lax.axis_index("y")}
    here = jnp.where(lax.axis_index("core") == 0, name[ways[0]], name[ways[1]])
    parts = [lax.dynamic_index_in_dim(value, (here + step) % 4, 0, keepdims=False) for step in (0, *steps)]
    total = parts[0]
    for step, part in zip(steps, parts[1:]):
        total = total + lax.ppermute(part, AXES, shifted(step, ways))
    return total


def shards(gamma, c_vir, c_occ, pair_list, shell_order):
    own_pair = lax.axis_index(("xh", "z", "y", "core"))
    where = jnp.stack([own_pair, lax.axis_index("xl"), lax.axis_index("core")]).astype(jnp.int32)
    keep0, send0, keep1, send1 = weighted_blocks(where, shell_order, pair_list.T, gamma[0], c_vir, c_occ)
    sums = []
    for keep, send in ((keep0, send0), (keep1, send1)):
        total = keep + lax.ppermute(send, "core", [(0, 1), (1, 0)])
        total = total.reshape(4, 32, *total.shape[1:])
        sums.append(exchanged(total, ("x", "y"), (1, 3, 2)))
    total = jnp.stack(sums, axis=1).reshape(4, 8, 2, SB, QUARTER)
    total = exchanged(total, ("y", "x"), (1, 3, 2))
    total = jnp.sum(lax.all_to_all(total, "z", 0, 0, tiled=True), axis=0)
    return total.transpose(0, 2, 1).reshape(2 * QUARTER, SB).astype(jnp.bfloat16)


def solution(mesh):
    inner = Mesh(mesh.devices.reshape(2, 8, 4, 2, 2), AXES)
    pair = ("xh", "z", "y", "core")
    return jax.shard_map(
        shards,
        mesh=inner,
        in_specs=(P(pair, "xl", None), P(), P(), P(), P()),
        out_specs=P("xl", pair),
        check_vma=False,
    )
```
